16 devices in a mesh: dz: 2 (over z), dy: 2 (over y), dx: 4 (over x, core).
Axes of the slice: x: 2, y: 2, z: 2, core: 2. Of those that a mesh axis runs over, the one named last changes fastest.
Arguments:
- x: bfloat16 [65536, 1024], P(('dx', 'dy', 'dz'))
- g: bfloat16 [65536, 1024], P(('dx', 'dy', 'dz'))
- w1: bfloat16 [1024, 4096], replicated
- w2: bfloat16 [4096, 1024], replicated
- w3: bfloat16 [1024, 4096], replicated
- w4: bfloat16 [4096, 1024], replicated
- m1: float32 [1024, 4096], P(('dx', 'dy', 'dz'))
- m2: float32 [4096, 1024], P(('dx', 'dy', 'dz'))
- m3: float32 [1024, 4096], P(('dx', 'dy', 'dz'))
- m4: float32 [4096, 1024], P(('dx', 'dy', 'dz'))
Outputs:
- output 1: bfloat16 [65536, 1024], P(('dx', 'dy', 'dz'))
- output 2: bfloat16 [1024, 4096], replicated
- output 3: bfloat16 [4096, 1024], replicated
- output 4: bfloat16 [1024, 4096], replicated
- output 5: bfloat16 [4096, 1024], replicated
- output 6: float32 [1024, 4096], P(('dx', 'dy', 'dz'))
- output 7: float32 [4096, 1024], P(('dx', 'dy', 'dz'))
- output 8: float32 [1024, 4096], P(('dx', 'dy', 'dz'))
- output 9: float32 [4096, 1024], P(('dx', 'dy', 'dz'))
All inputs are finite; a program needn't handle non-finite values.
Results may differ from the reference program's by a relative error of at most 0.0121176.
Values are sent between devices in bfloat16 or wider.
A program may use at most 1 GiB of HBM per device.

```python
import jax
import jax.numpy as jnp
from jax import lax

D = 1024
F = 4096
TOKENS_DEV = 4096
DEVICES = 16
TOKENS = TOKENS_DEV * DEVICES
LR = 0.0005
MU = 0.9


def setup_inputs(seed: int = 0) -> dict:
    ks = jax.random.split(jax.random.key(seed), 10)
    f32 = jnp.float32
    ms = 0.3 * (TOKENS_DEV / DEVICES) ** 0.5
    x = jax.random.normal(ks[0], (TOKENS, D), f32)
    g = jax.random.normal(ks[1], (TOKENS, D), f32)
    w1 = jax.random.normal(ks[2], (D, F), f32) * D ** -0.5
    w2 = jax.random.normal(ks[3], (F, D), f32) * F ** -0.5
    w3 = jax.random.normal(ks[4], (D, F), f32) * D ** -0.5
    w4 = jax.random.normal(ks[5], (F, D), f32) * F ** -0.5
    m1 = jax.random.normal(ks[6], (D, F), f32) * ms
    m2 = jax.random.normal(ks[7], (F, D), f32) * ms
    m3 = jax.random.normal(ks[8], (D, F), f32) * ms
    m4 = jax.random.normal(ks[9], (F, D), f32) * ms
    bf = jnp.bfloat16
    return {"x": x.astype(bf), "g": g.astype(bf), "w1": w1.astype(bf), "w2": w2.astype(bf),
            "w3": w3.astype(bf), "w4": w4.astype(bf), "m1": m1, "m2": m2, "m3": m3, "m4": m4}


def _gelu(z):
    return jax.nn.gelu(z, approximate=True)


def _gelu_grad(z, dh):
    return jax.vjp(_gelu, z.astype(jnp.float32))[1](dh.astype(jnp.float32))[0]


def _device_pass(x, g, w1, w2, w3, w4):
    f32, bf = jnp.float32, jnp.bfloat16
    z1 = jnp.dot(x, w1, preferred_element_type=f32).astype(bf)
    h1 = _gelu(z1.astype(f32)).astype(bf)
    h2 = (jnp.dot(h1, w2, preferred_element_type=f32) + x.astype(f32)).astype(bf)
    z3 = jnp.dot(h2, w3, preferred_element_type=f32).astype(bf)
    h3 = _gelu(z3.astype(f32)).astype(bf)
    s4 = jnp.dot(h3.T, g, preferred_element_type=f32)
    dh3 = jnp.dot(g, w4.T, preferred_element_type=f32).astype(bf)
    dz3 = _gelu_grad(z3, dh3).astype(bf)
    s3 = jnp.dot(h2.T, dz3, preferred_element_type=f32)
    dh2 = (jnp.dot(dz3, w3.T, preferred_element_type=f32) + g.astype(f32)).astype(bf)
    s2 = jnp.dot(h1.T, dh2, preferred_element_type=f32)
    dh1 = jnp.dot(dh2, w2.T, preferred_element_type=f32).astype(bf)
    dz1 = _gelu_grad(z1, dh1).astype(bf)
    s1 = jnp.dot(x.T, dz1, preferred_element_type=f32)
    dx = (jnp.dot(dz1, w1.T, preferred_element_type=f32) + dh2.astype(f32)).astype(bf)
    return dx, (s1, s2, s3, s4)


def reference(x, g, w1, w2, w3, w4, m1, m2, m3, m4):
    f32, bf = jnp.float32, jnp.bfloat16
    xs = x.reshape(DEVICES, TOKENS_DEV, D)
    gs = g.reshape(DEVICES, TOKENS_DEV, D)

    def step(acc, xg):
        dxd, ss = _device_pass(xg[0], xg[1], w1, w2, w3, w4)
        return tuple(a + s for a, s in zip(acc, ss)), dxd

    zeros = (jnp.zeros((D, F), f32), jnp.zeros((F, D), f32), jnp.zeros((D, F), f32), jnp.zeros((F, D), f32))
    acc, dxs = lax.scan(step, zeros, (xs, gs))
    m1n = MU * m1 + acc[0] / DEVICES
    m2n = MU * m2 + acc[1] / DEVICES
    m3n = MU * m3 + acc[2] / DEVICES
    m4n = MU * m4 + acc[3] / DEVICES
    w1n = (w1.astype(f32) - LR * m1n).astype(bf)
    w2n = (w2.astype(f32) - LR * m2n).astype(bf)
    w3n = (w3.astype(f32) - LR * m3n).astype(bf)
    w4n = (w4.astype(f32) - LR * m4n).astype(bf)
    dx = dxs.reshape(TOKENS, D)
    return (dx, w1n, w2n, w3n, w4n, m1n, m2n, m3n, m4n)
```

```python
import jax
import jax.numpy as jnp
from jax import lax
from jax.experimental import pallas as pl
from jax.experimental.pallas import tpu as pltpu
from jax.sharding import PartitionSpec as P

LR = 0.0005
MU = 0.9
DATA = ("dx", "dy", "dz")
C0 = 0.7978845608028654
C1 = 0.044715
T, D, F = 4096, 1024, 4096
BIG, HALF, QUART, GRP, BLK, CH = 1024, 512, 256, 128, 64, 16
f32, bf = jnp.float32, jnp.bfloat16
MESH = pl.DeviceIdType.MESH
VLIM = 63 * 2**20
NN = (((1,), (0,)), ((), ()))
NT = (((1,), (1,)), ((), ()))
TN = (((0,), (0,)), ((), ()))
CORE, SA, SB, SC, GY, GX, GZ, GC, GD = range(9)
DEPTH = {CORE: 3, SA: 3, SB: 3, SC: 3}
UNITS = 16
PART = 8
OFF_A = ((5, 8, 16, 21, 31, 34, 42, 51, 58), (4, 6, 13, 19, 28, 31, 38, 48, 60))
OFF_B = ((7, 8, 16, 21, 27, 32, 37, 44, 54), (7, 8, 14, 19, 23, 30, 33, 41, 51))


def _dot(a, b, dims):
    return lax.dot_general(a, b, dims, preferred_element_type=f32)


def _gelu_both(z):
    s = z * z
    t = jnp.tanh(z * (C0 + (C0 * C1) * s))
    w = 0.5 + 0.5 * t
    return z * w, w + (w * (1.0 - t)) * (z * (C0 + (3.0 * C0 * C1) * s))


def _gelu(z):
    return _gelu_both(z)[0]


def _gelu_grad(z):
    return _gelu_both(z)[1]


def _loop(n, body):
    def step(k, _):
        body(k)
        return 0
    lax.fori_loop(0, n, step, 0)


def _ds(start, size):
    return pl.ds(pl.multiple_of(start, size), size)


def _cut(k, size):
    return slice(k * size, (k + 1) * size)


def _fwd_kernel(x_ref, w1_ref, w2_ref, z1_ref, h1_ref, h2_ref):
    x = x_ref[...]
    for j in range(F // HALF):
        sl = _cut(j, HALF)
        z = jnp.dot(x, w1_ref[:, sl], preferred_element_type=f32).astype(bf)
        z1_ref[:, sl] = z
        h1_ref[:, sl] = _gelu(z.astype(f32)).astype(bf)
    h2 = jnp.dot(h1_ref[...], w2_ref[...], preferred_element_type=f32) + x.astype(f32)
    h2_ref[...] = h2.astype(bf)


def _row(m, n):
    return pl.BlockSpec((m, n), lambda i: (i, 0))


def _fwd(x, w1, w2):
    res = lambda s: pl.BlockSpec(s, lambda i: (0, 0), pipeline_mode=pl.Buffered(1))
    sh = lambda n: jax.ShapeDtypeStruct((T, n), bf)
    return pl.pallas_call(
        _fwd_kernel, grid=(T // HALF,),
        in_specs=[_row(HALF, D), res((D, F)), res((F, D))],
        out_specs=[_row(HALF, F), _row(HALF, F), _row(HALF, D)],
        out_shape=[sh(F), sh(F), sh(D)],
        compiler_params=pltpu.CompilerParams(vmem_limit_bytes=VLIM, dimension_semantics=("arbitrary",)),
        name="fwd")(x, w1, w2)


def _xor(a, b):
    return a + b - 2 * a * b


def _pick(s, a, b):
    return a + s * (b - a)


def _tile(t):
    return t % 2, (t // 2) % 2, t // 4


def _owner(t, i, j):
    g, be, ga = _tile(t)
    b, c = _xor(_xor(i, j), be), _xor(j, ga)
    return _pick(g, j, c), _pick(g, b, j), _pick(g, c, b)


def _block(x, c, y, z):
    return x * 8 + c * 4 + y * 2 + z


def _mid_kernel(x_h, g_h, w1_h, w2_h, w3_h, w4_h, m1_h, m2_h, m3_h, m4_h, z1_h, h1_h, h2_h,
                dz3_h, dz1_h, dx_h, wa_h, wb_h, ma_h, mb_h,
                R0, R1, TT, WA, WB, UA, UB, RcA, RcB, RaA, RaB, RbA, RbB, RdA, RdB,
                mA, wA, oA, mB, wB, oB, init_sem, w_sem, t_sem, o_sem, m_sem, ssem, rsem, gssem, grsem, cred):
    dx, my, mz = lax.axis_index("dx"), lax.axis_index("dy"), lax.axis_index("dz")
    mc, mx = dx % 2, dx // 2
    me = _block(mx, mc, my, mz)

    def dev(cc=0, x=0, y=0, z=0):
        return {"dx": _xor(mx, x) * 2 + _xor(mc, cc), "dy": _xor(my, y), "dz": _xor(mz, z)}

    core, devx, devy, devz = dev(cc=1), dev(x=1), dev(y=1), dev(z=1)
    ACROSS = {CORE: lambda col: core, SA: lambda col: dev(x=1 - col, y=col), SB: lambda col: dev(y=1 - col, z=col),
              SC: lambda col: dev(z=1 - col, x=col)}

    barrier = pltpu.get_barrier_semaphore()
    for d in (core, devx, devy, devz):
        pl.semaphore_signal(barrier, inc=1, device_id=d, device_id_type=MESH)
    pl.semaphore_wait(barrier, 4)

    def copies(pairs, sem):
        for a, b in pairs:
            pltpu.make_async_copy(a, b, sem).start()

    def landed(ref, sem):
        pltpu.make_async_copy(ref, ref, sem).wait()

    def cols(t):
        out = []
        for q in range(4):
            x, y, z = _owner(t, q // 2, q % 2)
            out.append(pl.multiple_of(_block(x, q // 2, y, z) * QUART + (t % 2) * GRP, GRP))
        return list(enumerate(out))

    def load_wa(t, w):
        s = t % 2
        copies([(w.at[:, pl.ds(c, GRP)], WA.at[s, :, _ds(GRP * q, GRP)]) for q, c in cols(t)], w_sem.at[0, s])

    def load_wb(t, w):
        s = t % 2
        copies([(w.at[pl.ds(c, GRP), :], WB.at[s, _ds(GRP * q, GRP), :]) for q, c in cols(t)], w_sem.at[1, s])

    def load_cols(t, a, k):
        copies([(a.at[:, pl.ds(c, GRP)], TT.at[k, :, _ds(GRP * q, GRP)]) for q, c in cols(t)], t_sem.at[k])

    def tile_in(k):
        landed(TT.at[k], t_sem.at[k])

    def store_cols(t, a):
        copies([(TT.at[1, :, _ds(GRP * q, GRP)], a.at[:, pl.ds(c, GRP)]) for q, c in cols(t)], o_sem.at[0])

    def stored():
        landed(TT.at[1], o_sem.at[0])

    def rc(ty, st, n, src, dst, d):
        s = n % DEPTH[st]
        return pltpu.make_async_remote_copy(src_ref=src, dst_ref=dst, send_sem=ssem.at[ty, st, s],
                                            recv_sem=rsem.at[ty, st, s], device_id=d, device_id_type=MESH)

    def gc(ty, st, n, ref, d):
        return pltpu.make_async_remote_copy(src_ref=ref, dst_ref=ref, send_sem=gssem.at[ty, st - GY, n],
                                            recv_sem=grsem.at[ty, st - GY, n], device_id=d, device_id_type=MESH)

    def take(ty, st, n):
        @pl.when(n >= DEPTH[st])
        def _():
            pl.semaphore_wait(cred.at[ty, st, n % DEPTH[st]], 1)

    def give(ty, st, n):
        m = n + DEPTH[st]

        @pl.when(m < UNITS)
        def _():
            pl.semaphore_signal(cred.at[ty, st, n % DEPTH[st]], inc=1, device_id=ACROSS[st](_xor(m % 2, ty)),
                                device_id_type=MESH)

    def add_rows(dst, src):
        def body(k):
            r = _ds(k * 2 * CH, 2 * CH)
            dst[r, :] = dst[r, :] + src[r, :]
        _loop(GRP // (2 * CH), body)

    def add_blocks(dst, src, count):
        def body(k):
            dst[k] = dst[k] + src[k]
        _loop(count, body)

    def update(m_ref, w_ref, o_ref, a_ref, b_ref, rows):
        def body(k):
            r = _ds(k * CH, CH)
            m = MU * m_ref[r, :] + (a_ref[r, :] + b_ref[r, :]) * (1.0 / UNITS)
            m_ref[r, :] = m
            o_ref[r, :] = (w_ref[r, :].astype(f32) - LR * m).astype(bf)
        _loop(rows // CH, body)

    def by_half(n, lo, hi):
        pl.when(n < PART)(lo)
        pl.when(n >= PART)(hi)

    def a_piece(n, i, z):
        g, be, ga = _tile(n % PART)
        j = _pick(g, _xor(z, ga), _xor(_xor(z, i), be))
        x, y, _ = _owner(n % PART, i, j)
        rows = pl.ds(pl.multiple_of(_block(x, i, y, z) * QUART + g * GRP, GRP), GRP)
        return wa_h.at[n // PART, rows, :], x, y

    def a_info(n):
        g, be, ga = _tile(n % PART)
        x, y, z = _owner(n % PART, mc, _pick(g, mx, my))
        snd = _pick(g, _xor(y, my), _xor(z, mz)) == 1
        last = _pick(g, _xor(z, mz), _xor(x, mx)) == 0
        keep = jnp.logical_not(snd)
        return snd, keep, keep & jnp.logical_not(last), keep & last

    def a_core(n):
        return rc(0, CORE, n, UA.at[pl.ds(2, 2)], RcA.at[n % DEPTH[CORE]], core)

    def a_sa(n):
        return rc(0, SA, n, RcA.at[n % DEPTH[CORE], 1], RaA.at[n % DEPTH[SA]], ACROSS[SA](n % 2))

    def a_sb(n):
        return rc(0, SB, n, RaA.at[n % DEPTH[SA]], RbA.at[n % DEPTH[SB]], ACROSS[SB](n % 2))

    def a_sc(n):
        return rc(0, SC, n, RbA.at[n % DEPTH[SB]], RdA.at[n % DEPTH[SC]], ACROSS[SC](n % 2))

    def a0(n):
        take(0, CORE, n)
        a_core(n).start()

    def a1(n):
        a_core(n).wait()
        for k in range(2):
            add_rows(RcA.at[n % DEPTH[CORE], k], UA.at[k])
        take(0, SA, n)
        a_sa(n).start()

    def a2(n):
        snd, keep, pas, fin = a_info(n)
        a_sa(n).wait()
        add_rows(RaA.at[n % DEPTH[SA]], RcA.at[n % DEPTH[CORE], 0])
        give(0, CORE, n)
        take(0, SB, n)
        pl.when(snd)(lambda: a_sb(n).start())

    def a3(n):
        snd, keep, pas, fin = a_info(n)
        pl.when(snd)(lambda: a_sb(n).wait_send())

        @pl.when(keep)
        def _():
            a_sb(n).wait_recv()
            add_rows(RbA.at[n % DEPTH[SB]], RaA.at[n % DEPTH[SA]])
        give(0, SA, n)
        take(0, SC, n)
        pl.when(pas)(lambda: a_sc(n).start())

        @pl.when(fin)
        def _():
            s = n % 2

            def load(m, w):
                pltpu.make_async_copy(m.at[_ds(s * GRP, GRP), :], mA.at[s], m_sem.at[0, 0, s]).start()
                pltpu.make_async_copy(w.at[pl.ds(pl.multiple_of(me * QUART + s * GRP, GRP), GRP), :], wA.at[s],
                                      m_sem.at[0, 1, s]).start()
            by_half(n, lambda: load(m4_h, w4_h), lambda: load(m2_h, w2_h))

    def a4(n):
        snd, keep, pas, fin = a_info(n)
        pl.when(pas)(lambda: a_sc(n).wait_send())

        @pl.when(fin)
        def _():
            s = n % 2
            a_sc(n).wait_recv()
            landed(mA.at[s], m_sem.at[0, 0, s])
            landed(wA.at[s], m_sem.at[0, 1, s])
            update(mA.at[s], wA.at[s], oA.at[s], RbA.at[n % DEPTH[SB]], RdA.at[n % DEPTH[SC]], GRP)
            out, _, _ = a_piece(n, mc, mz)
            pltpu.make_async_copy(mA.at[s], ma_h.at[n // PART, _ds(s * GRP, GRP), :], m_sem.at[0, 2, s]).start()
            pltpu.make_async_copy(oA.at[s], out, m_sem.at[0, 3, s]).start()
            pltpu.make_async_remote_copy(src_ref=oA.at[s], dst_ref=out, send_sem=gssem.at[0, 0, n],
                                         recv_sem=grsem.at[0, 0, n], device_id=devy, device_id_type=MESH).start()
        give(0, SB, n)
        give(0, SC, n)

    def a5(n):
        ref, x, y = a_piece(n, mc, mz)
        isx, isy = mx == x, my == y

        @pl.when(isx & isy)
        def _():
            s = n % 2
            gc(0, GY, n, ref, devy).wait_send()
            landed(mA.at[s], m_sem.at[0, 2, s])
            landed(oA.at[s], m_sem.at[0, 3, s])
        pl.when(isx & jnp.logical_not(isy))(lambda: gc(0, GY, n, ref, devy).wait_recv())
        pl.when(isx)(lambda: gc(0, GX, n, ref, devx).start())

    def a6(n):
        ref, x, y = a_piece(n, mc, mz)
        pl.when(mx == x)(lambda: gc(0, GX, n, ref, devx).wait_send())
        pl.when(mx != x)(lambda: gc(0, GX, n, ref, devx).wait_recv())
        gc(0, GZ, n, ref, devz).start()

    def a7(n):
        ref, _, _ = a_piece(n, mc, mz)
        gc(0, GZ, n, ref, devz).wait()
        gc(0, GC, n, ref, core).start()
        gc(0, GD, n, a_piece(n, mc, 1 - mz)[0], core).start()

    def a8(n):
        ref, _, _ = a_piece(n, mc, mz)
        gc(0, GC, n, ref, core).wait()
        gc(0, GD, n, ref, core).wait()

    def b_core(n):
        return rc(1, CORE, n, UB.at[pl.ds(8, 8)], RcB.at[n % DEPTH[CORE]], core)

    def b_sa(n):
        return rc(1, SA, n, RcB.at[n % DEPTH[CORE], pl.ds(4, 4)], RaB.at[n % DEPTH[SA]], ACROSS[SA](1 - n % 2))

    def b_sb(n):
        return rc(1, SB, n, RaB.at[n % DEPTH[SA], pl.ds(2, 2)], RbB.at[n % DEPTH[SB]], ACROSS[SB](1 - n % 2))

    def b_sc(n):
        return rc(1, SC, n, RbB.at[n % DEPTH[SB], 1], RdB.at[n % DEPTH[SC]], ACROSS[SC](1 - n % 2))

    def b_out(n, count):
        q = mc * 8 + mz * 4 + mx * 2 + my
        return wb_h.at[n // PART, n % PART, pl.ds(q // count * count, count)]

    def b0(n):
        take(1, CORE, n)
        b_core(n).start()

    def b1(n):
        b_core(n).wait()
        add_blocks(RcB.at[n % DEPTH[CORE]], UB, 8)
        take(1, SA, n)
        b_sa(n).start()

    def b2(n):
        b_sa(n).wait()
        add_blocks(RaB.at[n % DEPTH[SA]], RcB.at[n % DEPTH[CORE]], 4)
        give(1, CORE, n)
        take(1, SB, n)
        b_sb(n).start()

    def b3(n):
        b_sb(n).wait()
        add_blocks(RbB.at[n % DEPTH[SB]], RaB.at[n % DEPTH[SA]], 2)
        give(1, SA, n)
        take(1, SC, n)
        b_sc(n).start()
        s = n % 2

        def load(m, w):
            copies([(m.at[:, pl.ds(c, GRP)], mB.at[s, :, _ds(GRP * q, GRP)]) for q, c in cols(n % PART)],
                   m_sem.at[1, 0, s])
            copies([(w.at[_ds(me * BLK, BLK), pl.ds(c, GRP)], wB.at[s, :, _ds(GRP * q, GRP)])
                    for q, c in cols(n % PART)], m_sem.at[1, 1, s])
        by_half(n, lambda: load(m3_h, w3_h), lambda: load(m1_h, w1_h))

    def b4(n):
        s = n % 2
        b_sc(n).wait()
        landed(mB.at[s], m_sem.at[1, 0, s])
        landed(wB.at[s], m_sem.at[1, 1, s])
        update(mB.at[s], wB.at[s], oB.at[s, 0], RbB.at[n % DEPTH[SB], 0], RdB.at[n % DEPTH[SC]], BLK)
        copies([(mB.at[s, :, _ds(GRP * q, GRP)], mb_h.at[n // PART, :, pl.ds(c, GRP)]) for q, c in cols(n % PART)],
               m_sem.at[1, 2, s])
        pltpu.make_async_copy(oB.at[s], b_out(n, 1), m_sem.at[1, 3, s]).start()
        give(1, SB, n)
        give(1, SC, n)
        pltpu.make_async_remote_copy(src_ref=oB.at[s], dst_ref=b_out(n, 1), send_sem=gssem.at[1, 0, n],
                                     recv_sem=grsem.at[1, 0, n], device_id=devy, device_id_type=MESH).start()

    def b5(n):
        s = n % 2
        gc(1, GY, n, b_out(n, 1), devy).wait()
        landed(mB.at[s], m_sem.at[1, 2, s])
        landed(oB.at[s], m_sem.at[1, 3, s])
        gc(1, GX, n, b_out(n, 2), devx).start()

    def b6(n):
        gc(1, GX, n, b_out(n, 2), devx).wait()
        gc(1, GZ, n, b_out(n, 4), devz).start()

    def b7(n):
        gc(1, GZ, n, b_out(n, 4), devz).wait()
        gc(1, GC, n, b_out(n, 8), core).start()

    def b8(n):
        gc(1, GC, n, b_out(n, 8), core).wait()

    OPS = list(zip((a0, a1, a2, a3, a4, a5, a6, a7, a8), *OFF_A)) + list(zip((b0, b1, b2, b3, b4, b5, b6, b7, b8), *OFF_B))
    SPAN = max(max(o[1:]) for o in OPS)

    def exchange(v, k, lo, hi, v0, v1):
        for fn, first, second in sorted(OPS, key=lambda o: -o[1]):
            hits = []
            for off, s0, shift in ((first, 0, 0), (second, 10, 2)):
                lag, at = off // PART, off % PART
                if lo <= at < hi and v0 < s0 + PART + lag and v1 > s0 + lag:
                    hits.append(((v >= s0 + lag) & (v < s0 + PART + lag) & (k == at), v - lag - shift))
            if not hits:
                continue
            ok, n = hits[0]
            if len(hits) > 1:
                ok, n = ok | hits[1][0], jnp.where(ok, n, hits[1][1])
            pl.when(ok)(lambda fn=fn, n=n: fn(n))

    def s_rows(lhs, rhs, j, n):
        a = _pick(n % 2, mx, my)
        r = _dot(lhs[:, _ds(j * QUART, QUART)], rhs[...], TN)
        p = _xor(j, mc) * 2
        UA[p + a] = r[:GRP]
        UA[p + (1 - a)] = r[GRP:]

    def s_cols(lhs, rhs, j, n):
        col = 1 - n % 2
        r = _dot(lhs[:, _ds(j * HALF, HALF)], rhs[...], TN)
        px = _xor(j, mx)
        for k in range(PART):
            pc, py, pz = _xor(k // 4, mc), _xor((k // 2) % 2, my), _xor(k % 2, mz)
            UB[_block(pc, _pick(col, px, py), _pick(col, py, pz), _pick(col, pz, px))] = r[_cut(k, BLK)]

    def load_w_tiles(w, k0, dst):
        copies([(w.at[:, _ds(HALF * (k0 + k), HALF)], TT.at[dst, _ds(BIG * k, BIG), :]) for k in range(4)], t_sem.at[dst])

    def load_row_tile(a, i):
        d = 2 - i % 2
        copies([(a.at[_ds(HALF * i, HALF), _ds(HALF * k, HALF)], TT.at[d, _ds(HALF * k, HALF), :]) for k in range(PART)],
               t_sem.at[d])

    def row_tile(kk, a, add, out, then):
        i, hh = kk // 2, kk % 2
        d = 2 - i % 2

        @pl.when(hh == 0)
        def _():
            tile_in(d)
            pl.when(i < PART - 1)(lambda: load_row_tile(a, i + 1))
            pl.when(i == PART - 1)(then)
        rows, half = _ds(i * HALF, HALF), _ds(hh * HALF, HALF)
        acc = None
        for k in range(PART):
            w = TT[3 * (k // 4), _ds(BIG * (k % 4) + hh * HALF, HALF), :]
            p = _dot(TT[d, _cut(k, HALF), :], w, NT)
            acc = p if acc is None else acc + p
        out[rows, half] = (acc + add[rows, half].astype(f32)).astype(bf)

    load_wa(0, w3_h)
    load_wb(0, w4_h)
    for k in range(4):
        rows = _ds(k * BIG, BIG)
        pltpu.make_async_copy(h2_h.at[rows, :], R0.at[rows, :], init_sem.at[0, k]).start()
        pltpu.make_async_copy(g_h.at[rows, :], R1.at[rows, :], init_sem.at[1, k]).start()

    def step12(v):
        s = v % 2
        landed(WA.at[s], w_sem.at[0, s])
        landed(WB.at[s], w_sem.at[1, s])
        pl.when(v >= 1)(stored)
        pl.when(v == PART - 1)(lambda: load_w_tiles(w3_h, 4, 3))

        def d1(j):
            rows = _ds(j * BIG, BIG)

            @pl.when(v == 0)
            def _():
                landed(R0.at[rows, :], init_sem.at[0, j])
                landed(R1.at[rows, :], init_sem.at[1, j])
            z = _dot(R0[rows, :], WA[s], NN).astype(bf)
            dh = _dot(R1[rows, :], WB[s], NT).astype(bf)
            h, d = _gelu_both(z.astype(f32))
            TT[0, rows, :] = h.astype(bf)
            TT[1, rows, :] = (d * dh.astype(f32)).astype(bf)
            exchange(v, j, 0, 4, 0, 8)
        _loop(4, d1)
        store_cols(v, dz3_h)

        @pl.when(v < PART - 1)
        def _():
            load_wa(v + 1, w3_h)
            load_wb(v + 1, w4_h)

        def d2(j):
            s_rows(TT.at[0], R1, j, v)
            exchange(v, j + 4, 4, 6, 0, 8)
        _loop(2, d2)

        @pl.when(v == PART - 1)
        def _():
            load_w_tiles(w3_h, 0, 0)
            load_wb(0, w2_h)
            stored()
            load_row_tile(dz3_h, 0)

        def d3(j):
            s_cols(R0, TT.at[1], j, v)
            exchange(v, j + 6, 6, 8, 0, 8)
        _loop(2, d3)
    _loop(PART, step12)

    tile_in(0)
    tile_in(3)

    def step3(kk):
        row_tile(kk, dz3_h, R1, R0, lambda: load_cols(0, h1_h, 2))
        exchange(8 + kk // PART, kk % PART, 0, 8, 8, 10)
    _loop(2 * PART, step3)
    pltpu.make_async_copy(x_h, R1, o_sem.at[1]).start()
    load_cols(0, z1_h, 0)

    def step4(t):
        s = t % 2
        v = t + 10
        n = t + PART
        landed(WB.at[s], w_sem.at[1, s])
        tile_in(2 + s)
        pl.when(t < PART - 1)(lambda: load_cols(t + 1, h1_h, 3 - s))

        def d4(j):
            s_rows(TT.at[2 + s], R0, j, n)
            exchange(v, j, 0, 2, 10, 18)
        _loop(2, d4)
        pl.when(t == PART - 1)(lambda: load_w_tiles(w1_h, 4, 3))
        tile_in(0)
        pl.when(t >= 1)(stored)

        def d5(j):
            for q in range(4):
                rows = _ds(j * BIG + q * QUART, QUART)
                dh = _dot(R0[rows, :], WB[s], NT).astype(bf)
                d = _gelu_grad(TT[0, rows, :].astype(f32))
                TT[1, rows, :] = (d * dh.astype(f32)).astype(bf)
            exchange(v, j + 2, 2, 6, 10, 18)
        _loop(4, d5)
        store_cols(t, dz1_h)

        @pl.when(t < PART - 1)
        def _():
            load_cols(t + 1, z1_h, 0)
            load_wb(t + 1, w2_h)
        pl.when(t == 0)(lambda: landed(R1, o_sem.at[1]))
        pl.when(t == PART - 1)(lambda: load_w_tiles(w1_h, 0, 0))

        def d6(j):
            s_cols(R1, TT.at[1], j, n)

            @pl.when((t == PART - 1) & (j == 0))
            def _():
                stored()
                load_row_tile(dz1_h, 0)
            exchange(v, j + 6, 6, 8, 10, 18)
        _loop(2, d6)
    _loop(PART, step4)

    tile_in(0)
    tile_in(3)

    def step5(kk):
        pl.when(kk < 2 * PART)(lambda: row_tile(kk, dz1_h, R0, R1, lambda: None))
        pl.when(kk == 2 * PART)(lambda: pltpu.make_async_copy(R1, dx_h, o_sem.at[2]).start())
        exchange(18 + kk // PART, kk % PART, 0, 8, 18, 18 + SPAN)
    _loop(SPAN, step5)
    landed(R1, o_sem.at[2])


def _mid(x, g, w1, w2, w3, w4, m1, m2, m3, m4, z1, h1, h2):
    anyspec = pl.BlockSpec(memory_space=pl.ANY)
    sd = jax.ShapeDtypeStruct
    V, DMA = pltpu.VMEM, pltpu.SemaphoreType.DMA
    dc, da, db, dd = (DEPTH[k] for k in (CORE, SA, SB, SC))
    return pl.pallas_call(
        _mid_kernel,
        in_specs=[anyspec] * 13,
        out_specs=[anyspec] * 7,
        out_shape=[sd((T, F), bf), sd((T, F), bf), sd((T, D), bf),
                   sd((2, F, D), bf), sd((2, PART, UNITS, BLK, HALF), bf), sd((2, QUART, D), f32), sd((2, BLK, F), f32)],
        scratch_shapes=[
            V((T, D), bf), V((T, D), bf), V((4, T, HALF), bf), V((2, D, HALF), bf), V((2, HALF, D), bf),
            V((4, GRP, D), f32), V((UNITS, BLK, HALF), f32),
            V((dc, 2, GRP, D), f32), V((dc, 8, BLK, HALF), f32),
            V((da, GRP, D), f32), V((da, 4, BLK, HALF), f32),
            V((db, GRP, D), f32), V((db, 2, BLK, HALF), f32),
            V((dd, GRP, D), f32), V((dd, BLK, HALF), f32),
            V((2, GRP, D), f32), V((2, GRP, D), bf), V((2, GRP, D), bf),
            V((2, BLK, HALF), f32), V((2, BLK, HALF), bf), V((2, 1, BLK, HALF), bf),
            DMA((2, 4)), DMA((2, 2)), DMA((4,)), DMA((3,)), DMA((2, 4, 2)),
            DMA((2, 4, dc)), DMA((2, 4, dc)), DMA((2, 5, UNITS)), DMA((2, 5, UNITS)),
            pltpu.SemaphoreType.REGULAR((2, 4, dc)),
        ],
        compiler_params=pltpu.CompilerParams(vmem_limit_bytes=VLIM, collective_id=0, has_side_effects=True),
        name="mid")(x, g, w1, w2, w3, w4, m1, m2, m3, m4, z1, h1, h2)


def _last_kernel(dx, wa1, wb1, wa0, wb0, ma1, mb1, ma0, mb0, dxn, w2n, w1n, w4n, w3n, m2n, m1n, m4n, m3n):
    dxn[...] = dx[...]
    for src, dst in ((wa1, w2n), (wa0, w4n), (ma1, m2n), (ma0, m4n), (mb1, m1n), (mb0, m3n)):
        dst[...] = src[0]
    for src, dst in ((wb1, w1n), (wb0, w3n)):
        for t in range(PART):
            for q in range(4):
                x, y, z = _owner(t, q // 2, q % 2)
                k = 2 * _block(x, q // 2, y, z) + t % 2
                dst[:, _cut(k, GRP)] = src[0, t, 0, :, _cut(q, GRP)]


def _last(dx, wa, wb, ma, mb):
    sd = jax.ShapeDtypeStruct
    col = lambda m, n: pl.BlockSpec((m, n), lambda i: (0, i))
    half = lambda h, m, n: pl.BlockSpec((1, m, n), lambda i: (h, i, 0))
    hcol = lambda h, m, n: pl.BlockSpec((1, m, n), lambda i: (h, 0, i))
    blk = lambda h: pl.BlockSpec((1, PART, 1, BLK, HALF), lambda i: (
        h, 0, (i // 4) % 2 * 8 + i % 2 * 4 + i // 8 * 2 + (i // 2) % 2, 0, 0))
    ins, outs, shapes = [_row(QUART, D)], [_row(QUART, D)], [sd((T, D), bf)]
    for h in (1, 0):
        ins += [half(h, QUART, D), blk(h)]
        outs += [_row(QUART, D), _row(BLK, F)]
        shapes += [sd((F, D), bf), sd((D, F), bf)]
    for h in (1, 0):
        ins += [half(h, CH, D), hcol(h, BLK, QUART)]
        outs += [_row(CH, D), col(BLK, QUART)]
        shapes += [sd((QUART, D), f32), sd((BLK, F), f32)]
    return pl.pallas_call(
        _last_kernel, grid=(UNITS,), in_specs=ins, out_specs=outs, out_shape=shapes,
        compiler_params=pltpu.CompilerParams(vmem_limit_bytes=VLIM, dimension_semantics=("arbitrary",)),
        name="last")(dx, wa, wb, wa, wb, ma, mb, ma, mb)


def solution(mesh):
    def local(x, g, w1, w2, w3, w4, m1, m2, m3, m4):
        z1, h1, h2 = _fwd(x, w1, w2)
        _, _, dx, wa, wb, ma, mb = _mid(x, g, w1, w2, w3, w4, m1, m2, m3, m4, z1, h1, h2)
        dx, w2n, w1n, w4n, w3n, m2n, m1n, m4n, m3n = _last(dx, wa, wb, ma, mb)
        return dx, w1n, w2n, w3n, w4n, m1n, m2n, m3n, m4n

    row, rep = P(DATA, None), P()
    return jax.shard_map(local, mesh=mesh,
                         in_specs=(row, row, rep, rep, rep, rep, row, row, row, row),
                         out_specs=(row, rep, rep, rep, rep, row, row, row, row),
                         check_vma=False)
```
